32 devices in a mesh: seq: 16 (over z, y, core), res: 2 (over x).
Axes of the slice: x: 2, y: 2, z: 4, core: 2. Of those that a mesh axis runs over, the one named last changes fastest.
Arguments:
- homolog_embedding: bfloat16 [256, 128, 256], P('seq', 'res'), may hold values from -6 to 6
- pair_features: bfloat16 [128, 128, 128], P('seq', 'res'), may hold values from -6 to 6
- row_present_mask: int32 [256], replicated, may hold values 0 or 1
- residue_keep_mask: int32 [128], replicated, may hold values 0 or 1
- query_weight: bfloat16 [256, 256], replicated, may hold values from -64 to 64
- key_weight: bfloat16 [256, 256], replicated, may hold values from -1 to 1
- content_matrix: bfloat16 [256, 256], replicated, may hold values from -0.375 to 0.375
- sigmoid_switch_matrix: bfloat16 [256, 256], replicated, may hold values from -0.375 to 0.375
- focus_merge_matrix: bfloat16 [256, 256], replicated, may hold values from -0.375 to 0.375
- widening_matrix: bfloat16 [256, 1024], replicated, may hold values from -0.375 to 0.375
- narrowing_matrix: bfloat16 [1024, 256], replicated, may hold values from -0.1875 to 0.1875
- first_factor_matrix: bfloat16 [256, 32], replicated, may hold values from -0.375 to 0.375
- second_factor_matrix: bfloat16 [256, 32], replicated, may hold values from -0.375 to 0.375
- outer_product_weight: bfloat16 [1024, 128], replicated, may hold values from -1 to 1
- outer_product_bias: float32 [128], replicated, may hold values from -3 to 3
- pair_up_weight: bfloat16 [128, 512], replicated, may hold values from -0.5 to 0.5
- pair_down_weight: bfloat16 [512, 128], replicated, may hold values from -0.25 to 0.25
Outputs:
- msa_update: bfloat16 [256, 128, 256], P('seq', 'res')
- pair_update: bfloat16 [128, 128, 128], P('seq', 'res')
The draws below stay inside these ranges and needn't reach their ends.
All inputs are finite; a program needn't handle non-finite values.
Results may differ from the reference program's by a relative error of at most 0.012.
Values may be sent and summed in bfloat16 or wider, within the bound.
A program may use at most 64 MiB of HBM per device.

```python
import math
import jax
import jax.numpy as jnp
from jax import lax

EMBED_BREADTH = 256
C_Z = 128
FOCUS_NUMBER = 8
FOCUS_BREADTH = 32
COUPLING_DIM = 32
LAYER_HIDDEN = 1024
TRANS_Z = 512
HOMOLOG_NUMBER = 256
AMINO_NUMBER = 128


def query_key_base(key):
    base_key = jax.random.fold_in(key, 7)
    asking_random_seed, lookup_random_seed = jax.random.split(base_key, 2)
    asking_piece = jax.random.normal(asking_random_seed, (EMBED_BREADTH, FOCUS_NUMBER * FOCUS_BREADTH), jnp.float32) / math.sqrt(EMBED_BREADTH)
    lookup_piece = jax.random.normal(lookup_random_seed, (EMBED_BREADTH, FOCUS_NUMBER * FOCUS_BREADTH), jnp.float32) / math.sqrt(EMBED_BREADTH)
    lookup_piece = jnp.clip(lookup_piece, -0.9, 0.9)
    asking_piece = jnp.clip(asking_piece, -0.9, 0.9)
    return (asking_piece, lookup_piece)


def draw_key_weight(key, part):
    asking_piece, lookup_piece = query_key_base(key)
    return lookup_piece.astype(jnp.bfloat16)


def draw_query_weight(key, part):
    asking_piece, lookup_piece = query_key_base(key)
    return asking_piece.astype(jnp.bfloat16)


def touch_ends(drawn, stream_key, least, high):
    longest = drawn.shape.index(max(drawn.shape))
    spots = []
    for shift in (0, 1):
        where = [jax.random.randint(jax.random.fold_in(stream_key, axis), (), 0, length) for axis, length in enumerate(drawn.shape)]
        where[longest] = (where[longest] + shift) % drawn.shape[longest]
        spots.append(tuple(where))
    return drawn.at[spots[0]].set(least).at[spots[1]].set(high)


def levels(rng, dims, shards, smallest, top_value):
    level, own = 1.0, jax.random.fold_in(rng, 6)
    for axis_at, shards_of in shards:
        heights = jnp.exp(jax.random.uniform(jax.random.fold_in(own, axis_at), (shards_of,), jnp.float32, smallest / len(shards), top_value / len(shards)))
        level = level * jnp.repeat(heights, dims[axis_at] // shards_of).reshape([-1 if axis == axis_at else 1 for axis in range(len(dims))])
    return level


def scatter_about(stream_key, extent, scale, reach, cuts=(), kind=jnp.bfloat16):
    drawn = scale * jax.random.normal(stream_key, extent, jnp.float32)
    if cuts:
        drawn = drawn * levels(stream_key, extent, cuts, -0.22, 0.18)
    return jnp.clip(drawn, -reach, reach).astype(kind)


def setup_inputs(seed: int = 0) -> dict:
    streams_of = jax.random.split(jax.random.key(seed), 18)
    return {
        "homolog_embedding": scatter_about(streams_of[0], (HOMOLOG_NUMBER, AMINO_NUMBER, EMBED_BREADTH), 1.0, 6.0, ((0, 16), (1, 2))),
        "pair_features": scatter_about(streams_of[1], (AMINO_NUMBER, AMINO_NUMBER, C_Z), 1.0, 6.0, ((0, 16), (1, 2))),
        "row_present_mask": touch_ends((jax.random.randint(streams_of[2], (HOMOLOG_NUMBER,), 0, 8) < 7).astype(jnp.int32), jax.random.fold_in(streams_of[2], 1), 0, 1),
        "residue_keep_mask": touch_ends((jax.random.randint(streams_of[3], (AMINO_NUMBER,), 0, 8) < 7).astype(jnp.int32), jax.random.fold_in(streams_of[3], 1), 0, 1),
        "query_weight": draw_query_weight(jax.random.fold_in(streams_of[17], 71), 0),
        "key_weight": draw_key_weight(jax.random.fold_in(streams_of[17], 71), 0),
        "content_matrix": scatter_about(streams_of[6], (EMBED_BREADTH, FOCUS_NUMBER * FOCUS_BREADTH), EMBED_BREADTH ** -0.5, 0.375),
        "sigmoid_switch_matrix": scatter_about(streams_of[7], (EMBED_BREADTH, FOCUS_NUMBER * FOCUS_BREADTH), EMBED_BREADTH ** -0.5, 0.375),
        "focus_merge_matrix": scatter_about(streams_of[8], (FOCUS_NUMBER * FOCUS_BREADTH, EMBED_BREADTH), (FOCUS_NUMBER * FOCUS_BREADTH) ** -0.5, 0.375),
        "widening_matrix": scatter_about(streams_of[9], (EMBED_BREADTH, LAYER_HIDDEN), EMBED_BREADTH ** -0.5, 0.375),
        "narrowing_matrix": scatter_about(streams_of[10], (LAYER_HIDDEN, EMBED_BREADTH), LAYER_HIDDEN ** -0.5, 0.1875),
        "first_factor_matrix": scatter_about(streams_of[11], (EMBED_BREADTH, COUPLING_DIM), EMBED_BREADTH ** -0.5, 0.375),
        "second_factor_matrix": scatter_about(streams_of[12], (EMBED_BREADTH, COUPLING_DIM), EMBED_BREADTH ** -0.5, 0.375),
        "outer_product_weight": scatter_about(streams_of[13], (COUPLING_DIM * COUPLING_DIM, C_Z), COUPLING_DIM ** -0.5, 1.0),
        "outer_product_bias": scatter_about(streams_of[14], (C_Z,), 0.5, 3.0, (), jnp.float32),
        "pair_up_weight": scatter_about(streams_of[15], (C_Z, TRANS_Z), C_Z ** -0.5, 0.5),
        "pair_down_weight": scatter_about(streams_of[16], (TRANS_Z, C_Z), TRANS_Z ** -0.5, 0.25),
    }


epsilon = 1e-05
mask_fill = 1000000000.0

def layer_norm(values):
    centre = values - lax.optimization_barrier(jnp.mean(values, axis=-1, keepdims=True))
    spread = lax.optimization_barrier(jnp.mean(centre * centre, axis=-1, keepdims=True))
    return centre * lax.rsqrt(spread + epsilon)

def column_delta(block, row_present_flags, attention_weights):
    query_weight, key_weight, content_matrix, sigmoid_switch_matrix, focus_merge_matrix, widening_matrix, narrowing_matrix, first_factor_matrix, second_factor_matrix = attention_weights
    row_count, item_count, channel_width = block.shape
    inputs = block.astype(jnp.float32)
    normed = layer_norm(inputs).astype(jnp.bfloat16)
    scaling = 1.0 / math.sqrt(FOCUS_BREADTH)
    queries = (jnp.dot(normed, query_weight, preferred_element_type=jnp.float32) * scaling).astype(jnp.bfloat16)
    queries = queries.reshape(row_count, item_count, FOCUS_NUMBER, FOCUS_BREADTH)
    keys_all = jnp.dot(normed, key_weight, preferred_element_type=jnp.float32).astype(jnp.bfloat16)
    keys_all = keys_all.reshape(row_count, item_count, FOCUS_NUMBER, FOCUS_BREADTH)
    values_all = jnp.dot(normed, content_matrix, preferred_element_type=jnp.float32).astype(jnp.bfloat16)
    values_all = values_all.reshape(row_count, item_count, FOCUS_NUMBER, FOCUS_BREADTH)
    gate_values = jax.nn.sigmoid(jnp.dot(normed, sigmoid_switch_matrix, preferred_element_type=jnp.float32))
    scores = jnp.einsum('skhd,tkhd->khst', queries.astype(jnp.float32), keys_all.astype(jnp.float32))
    scores = scores + ((row_present_flags - 1.0) * mask_fill)[None, None, None, :]
    peak_score = lax.optimization_barrier(jnp.max(scores, axis=-1, keepdims=True))
    exponent = jnp.exp(scores - peak_score)
    probs = (exponent / lax.optimization_barrier(jnp.sum(exponent, axis=-1, keepdims=True))).astype(jnp.bfloat16)
    attended = jnp.einsum('khst,tkhd->skhd', probs.astype(jnp.float32), values_all.astype(jnp.float32))
    attended = attended.reshape(row_count, item_count, FOCUS_NUMBER * FOCUS_BREADTH)
    gated = (gate_values * attended).astype(jnp.bfloat16)
    after_attn = (inputs + jnp.dot(gated, focus_merge_matrix, preferred_element_type=jnp.float32)).astype(jnp.bfloat16)
    normed_two = layer_norm(after_attn.astype(jnp.float32)).astype(jnp.bfloat16)
    hidden = jax.nn.relu(jnp.dot(normed_two, widening_matrix, preferred_element_type=jnp.float32)).astype(jnp.bfloat16)
    after_trans = (after_attn.astype(jnp.float32) + jnp.dot(hidden, narrowing_matrix, preferred_element_type=jnp.float32)).astype(jnp.bfloat16)
    normed_three = layer_norm(after_trans.astype(jnp.float32)).astype(jnp.bfloat16)
    row_scale = row_present_flags[:, None, None]
    left_proj = (jnp.dot(normed_three, first_factor_matrix, preferred_element_type=jnp.float32) * row_scale).astype(jnp.bfloat16)
    right_proj = (jnp.dot(normed_three, second_factor_matrix, preferred_element_type=jnp.float32) * row_scale).astype(jnp.bfloat16)
    return (after_trans, left_proj, right_proj)

def pair_block_update(left_rows, right_full, pair_block, norm_block, outer_product_weight, outer_product_bias, pair_up_weight, pair_down_weight):
    outer = jnp.einsum('sic,sje->ijce', left_rows.astype(jnp.float32), right_full.astype(jnp.float32)).astype(jnp.bfloat16)
    row_span, column_extent = norm_block.shape
    flat = outer.reshape(row_span, column_extent, COUPLING_DIM * COUPLING_DIM)
    projected = jnp.dot(flat, outer_product_weight, preferred_element_type=jnp.float32) + outer_product_bias
    outer_mean = projected / jnp.maximum(norm_block, 1.0)[:, :, None]
    pair_mid = (pair_block.astype(jnp.float32) + outer_mean).astype(jnp.bfloat16)
    normed = layer_norm(pair_mid.astype(jnp.float32)).astype(jnp.bfloat16)
    hidden = jax.nn.relu(jnp.dot(normed, pair_up_weight, preferred_element_type=jnp.float32)).astype(jnp.bfloat16)
    return (pair_mid.astype(jnp.float32) + jnp.dot(hidden, pair_down_weight, preferred_element_type=jnp.float32)).astype(jnp.bfloat16)

def reference(homolog_embedding, pair_features, row_present_mask, residue_keep_mask, query_weight, key_weight, content_matrix, sigmoid_switch_matrix, focus_merge_matrix, widening_matrix, narrowing_matrix, first_factor_matrix, second_factor_matrix, outer_product_weight, outer_product_bias, pair_up_weight, pair_down_weight):
    row_present_flags = row_present_mask.astype(jnp.float32)
    res_flags = residue_keep_mask.astype(jnp.float32)
    overall_rows, residue_total, channel_width = homolog_embedding.shape
    column_tile = math.gcd(residue_total, 64)
    group_view = homolog_embedding.reshape(overall_rows, residue_total // column_tile, column_tile, channel_width).transpose(1, 0, 2, 3)
    attention_weights = (query_weight, key_weight, content_matrix, sigmoid_switch_matrix, focus_merge_matrix, widening_matrix, narrowing_matrix, first_factor_matrix, second_factor_matrix)

    def group_size(block):
        return column_delta(block, row_present_flags, attention_weights)
    alignment_output, left_full, right_full = lax.map(group_size, group_view)
    alignment_output = alignment_output.transpose(1, 0, 2, 3).reshape(overall_rows, residue_total, channel_width)
    left_full = left_full.transpose(1, 0, 2, 3).reshape(overall_rows, residue_total, COUPLING_DIM)
    right_full = right_full.transpose(1, 0, 2, 3).reshape(overall_rows, residue_total, COUPLING_DIM)
    res_half = residue_keep_mask.astype(jnp.bfloat16)
    left_full = left_full * res_half[None, :, None]
    right_full = right_full * res_half[None, :, None]
    live_rows = jnp.sum(row_present_flags)
    row_block = math.gcd(residue_total, 32)
    block_count = residue_total // row_block
    left_groups = left_full.reshape(overall_rows, block_count, row_block, COUPLING_DIM).transpose(1, 0, 2, 3)
    pair_groups = pair_features.reshape(block_count, row_block, residue_total, C_Z)
    norm_groups = live_rows * res_flags.reshape(block_count, row_block)[:, :, None] * res_flags[None, None, :]

    def per_rows(pieces):
        left_rows, pair_block, norm_block = pieces
        return pair_block_update(left_rows, right_full, pair_block, norm_block, outer_product_weight, outer_product_bias, pair_up_weight, pair_down_weight)
    pair_output = lax.map(per_rows, (left_groups, pair_groups, norm_groups)).reshape(residue_total, residue_total, C_Z)
    return (alignment_output, pair_output)
```

```python
import functools
import math

import jax
import jax.numpy as jnp
from jax import lax
from jax.experimental import pallas as pl
from jax.experimental.pallas import tpu as pltpu
from jax.sharding import PartitionSpec as P

FOCUS_NUMBER = 8
FOCUS_BREADTH = 32
COUPLING_DIM = 32
OWNED = 4
PACK = 4

epsilon = 1e-05
mask_fill = 1000000000.0
F32 = jnp.float32
BF16 = jnp.bfloat16


def layer_norm(values):
    centre = values - jnp.mean(values, axis=-1, keepdims=True)
    spread = jnp.mean(centre * centre, axis=-1, keepdims=True)
    return centre * lax.rsqrt(spread + epsilon)


def mm(a, b):
    return jnp.dot(a, b, preferred_element_type=F32)


def mm_nt(a, b):
    return lax.dot_general(a, b, (((1,), (1,)), ((), ())), preferred_element_type=F32)


def kernel(
    n,
    res_n,
    x_ref,
    pair_ref,
    rowm_ref,
    keep_ref,
    wq,
    wk,
    wv,
    wg,
    wm,
    wu,
    wn,
    w1,
    w2,
    wo,
    bias_ref,
    wpu,
    wpd,
    msa_out,
    pair_out,
    proj_w,
    wm_v,
    wu_v,
    wn_v,
    w1_v,
    w2_v,
    wo_v,
    wpu_v,
    wpd_v,
    xcol,
    ycol,
    n3,
    lsend,
    lbuf,
    lexp,
    rbuf,
    keepj,
    w_sem,
    own_sem,
    in_send,
    in_recv,
    l_send,
    l_recv,
    r_send,
    rz_recv,
    ry_recv,
    rc_recv,
    o_send,
    o_recv,
):
    me = lax.axis_index("seq")
    my_res = lax.axis_index("res")
    cols, shard_rows, width = x_ref.shape
    rows = n * shard_rows
    lines = n // 4
    row_span = pair_ref.shape[0]

    def remote(src, dst, send, recv, where):
        return pltpu.make_async_remote_copy(
            src_ref=src,
            dst_ref=dst,
            send_sem=send,
            recv_sem=recv,
            device_id=where,
            device_id_type=pl.DeviceIdType.MESH,
        )

    def at(s):
        return (s, my_res)

    def drain(ref, sem):
        pltpu.make_async_copy(ref, ref, sem).wait()

    my_rows = pl.ds(pl.multiple_of(me * shard_rows, shard_rows), shard_rows)
    for c in range(OWNED):

        @pl.loop(1, n)
        def _(k, c=c):
            dst = lax.rem(me + k, n)
            remote(
                x_ref.at[dst * OWNED + c],
                xcol.at[c, my_rows],
                in_send.at[c],
                in_recv.at[c],
                at(dst),
            ).start()

    own = pltpu.make_async_copy(
        x_ref.at[pl.ds(me * OWNED, OWNED)], xcol.at[:, my_rows], own_sem
    )
    own.start()
    fetches = [
        (wq, proj_w.at[:, 0:width]),
        (wk, proj_w.at[:, width : 2 * width]),
        (wv, proj_w.at[:, 2 * width : 3 * width]),
        (wg, proj_w.at[:, 3 * width : 4 * width]),
        (wm, wm_v),
        (wu, wu_v),
        (wn, wn_v),
        (w1, w1_v),
        (w2, w2_v),
        (wo, wo_v),
        (wpu, wpu_v),
        (wpd, wpd_v),
    ]
    fetches = [pltpu.make_async_copy(s, d, w_sem.at[i]) for i, (s, d) in enumerate(fetches)]
    for f in fetches:
        f.start()

    sub = lax.broadcasted_iota(jnp.int32, (8, 128), 0)
    for d in range(n):
        flags = [
            keep_ref[my_res * cols + d * OWNED + m].astype(F32) for m in range(OWNED)
        ]
        tile = jnp.full((8, 128), flags[0], F32)
        for m in range(1, OWNED):
            tile = jnp.where(lax.rem(sub, OWNED) == m, flags[m], tile)
        keepj[d] = tile

    row_flags = rowm_ref[...].astype(F32)
    bias = (row_flags - 1.0) * mask_fill
    lane = lax.broadcasted_iota(jnp.int32, (1, width), 1)
    head_masks = [
        (lane // FOCUS_BREADTH == h).astype(F32).astype(BF16) for h in range(FOCUS_NUMBER)
    ]
    scaling = 1.0 / math.sqrt(FOCUS_BREADTH)
    own.wait()
    for f in fetches:
        f.wait()

    def column(c, carry):
        drain(xcol.at[c, pl.ds(0, (n - 1) * shard_rows)], in_recv.at[c])
        inputs = xcol[c].astype(F32)
        normed = layer_norm(inputs).astype(BF16)
        q = (mm(normed, proj_w[:, 0:width]) * scaling).astype(BF16)
        k = mm(normed, proj_w[:, width : 2 * width]).astype(BF16)
        v = mm(normed, proj_w[:, 2 * width : 3 * width]).astype(BF16)
        top = jnp.zeros((rows, width), F32)
        low = jnp.zeros((rows, width), F32)
        for h in range(FOCUS_NUMBER):
            scores = mm_nt(q * head_masks[h], k) + bias
            peak = jnp.max(scores, axis=-1, keepdims=True)
            e = jnp.exp(scores - peak).astype(BF16)
            top = top + mm(e, v * head_masks[h])
            low = low + mm(e, jnp.broadcast_to(head_masks[h], (rows, width)))
        gate = jax.nn.sigmoid(mm(normed, proj_w[:, 3 * width : 4 * width]))
        gated = (gate * (top / low)).astype(BF16)
        after = (inputs + mm(gated, wm_v[...])).astype(BF16)
        normed_two = layer_norm(after.astype(F32)).astype(BF16)
        hidden = jnp.maximum(mm(normed_two, wu_v[...]), 0.0).astype(BF16)
        updated = (after.astype(F32) + mm(hidden, wn_v[...])).astype(BF16)
        ycol[c] = updated
        n3[c] = layer_norm(updated.astype(F32)).astype(BF16)
        return carry

    lax.fori_loop(0, OWNED, column, 0)

    lanes = lax.broadcasted_iota(jnp.int32, (1, 128), 1)
    tall = lax.broadcasted_iota(jnp.int32, (128, width), 0)
    left = jnp.zeros((rows, 128), F32)
    right = jnp.zeros((128, rows), F32)
    for c in range(OWNED):
        here = (lanes // COUPLING_DIM == c).astype(F32).astype(BF16)
        left = left + mm(n3[c], w1_v[...] * here)
        there = (lax.rem(tall, OWNED) == c).astype(F32).astype(BF16)
        right = right + mm_nt(w2_v[...] * there, n3[c])
    right = (right * row_flags).astype(BF16)
    my_block = pl.ds(pl.multiple_of(me * 32, 32), 32)
    for k in range(PACK):
        rbuf[k, my_block, :] = right[k * 32 : (k + 1) * 32]
    lsend[...] = left.astype(BF16)

    line = me // 4
    spot = lax.rem(me, 4)
    core = lax.rem(me, 2)
    y_pair = line * 4 + lax.rem(spot + 2, 4)
    c_pair = me + 1 - 2 * core

    def pass_on(block, sem, to):
        part = rbuf.at[:, pl.ds(pl.multiple_of(block * 32, 32), 32)]
        remote(part, part, r_send, sem, at(to)).start()

    def got(block, sem):
        drain(rbuf.at[:, pl.ds(pl.multiple_of(block * 32, 32), 32)], sem)

    def line_block(k):
        z = lax.rem(line + lines - k, lines)
        return z, z * 4 + spot, z * 4 + lax.rem(spot + 2, 4)

    for k in range(1, lines):
        pass_on(me, rz_recv.at[line], lax.rem(line + k, lines) * 4 + spot)
    pass_on(me, ry_recv.at[line], y_pair)
    pass_on(me, rc_recv.at[0, line], c_pair)

    q_row = my_res * (n // res_n) + me // res_n
    slot = lax.rem(me, res_n)
    for r in range(res_n):
        local = jnp.logical_and(q_row == me, my_res == r)

        @pl.when(local)
        def _():
            pltpu.make_async_copy(lsend, lbuf.at[slot], l_recv.at[slot]).start()

        @pl.when(jnp.logical_not(local))
        def _(r=r):
            remote(lsend, lbuf.at[slot], l_send.at[r], l_recv.at[slot], (q_row, r)).start()

    for k in range(1, lines):
        z, block, _ = line_block(k)
        got(block, rz_recv.at[z])
        pass_on(block, ry_recv.at[z], y_pair)
        pass_on(block, rc_recv.at[0, z], c_pair)
    for k in range(lines):
        z, _, block = line_block(k)
        got(block, ry_recv.at[z])
        pass_on(block, rc_recv.at[1, z], c_pair)

    @pl.loop(1, n)
    def _(k):
        dst = lax.rem(me + k, n)
        remote(
            ycol.at[:, pl.ds(pl.multiple_of(dst * shard_rows, shard_rows), shard_rows)],
            msa_out.at[pl.ds(me * OWNED, OWNED)],
            o_send,
            o_recv,
            at(dst),
        ).start()

    home = pltpu.make_async_copy(
        ycol.at[:, my_rows], msa_out.at[pl.ds(me * OWNED, OWNED)], own_sem
    )
    home.start()

    for t in range(res_n):
        drain(lbuf.at[t], l_recv.at[t])
        block = lbuf[t].astype(F32)
        turned = [block] + [pltpu.roll(block, 32 * a, 1) for a in range(1, PACK)]
        for k in range(PACK):
            inside = lanes // COUPLING_DIM == k
            for m in range(OWNED):
                tile = jnp.where(inside, turned[(k - m) % PACK], 0.0).astype(BF16)
                i = t * OWNED + m
                lexp[k, :, i * 128 : (i + 1) * 128] = tile
    for k in range(lines):
        z, block, other = line_block(k)
        got(z * 4 + lax.rem(spot, 4) + 1 - 2 * core, rc_recv.at[0, z])
        got(z * 4 + lax.rem(spot + 2, 4) + 1 - 2 * core, rc_recv.at[1, z])

    live = jnp.sum(row_flags, axis=-1, keepdims=True)
    sub3 = lax.broadcasted_iota(jnp.int32, (1, 8, 128), 1)
    first = sub3 < 4
    flags_j = keepj[...]
    add_bias = bias_ref[...].reshape(1, 1, 128)
    half = n // 2

    def pair_rows(a, b):
        return jnp.where(first, a, pltpu.roll(b, 4, 1)), jnp.where(first, pltpu.roll(a, 4, 1), b)

    for ip in range(row_span // 2):
        outer = jnp.zeros((n * 32, 256), F32)
        for k in range(PACK):
            outer = outer + mm(rbuf[k], lexp[k, :, ip * 256 : (ip + 1) * 256])
        outer = outer.reshape(n, 4, 8, 256)
        sums = []
        for p in range(2):
            total = jnp.zeros((n * 8, 256), F32)
            for g in range(4):
                piece = outer[:, g, :, p * 128 : (p + 1) * 128].reshape(n * 8, 128).astype(BF16)
                total = total + mm(piece, wo_v[g * 128 : (g + 1) * 128, :])
            total = total.reshape(n, 8, 256)
            total = jnp.where(first, total[:, :, :128], total[:, :, 128:])
            sums.append(total + pltpu.roll(total, 4, 1))
        total = jnp.where(first, sums[0], sums[1])
        i = 2 * ip
        keep_a = keep_ref[me * row_span + i].astype(F32)
        keep_b = keep_ref[me * row_span + i + 1].astype(F32)
        flags = jnp.where(first, keep_a, keep_b) * flags_j
        norm = live.reshape(1, 1, 1) * flags
        mean = (total * flags + add_bias) / jnp.maximum(norm, 1.0)
        a = pair_ref[i].astype(F32).reshape(half, 8, 128)
        b = pair_ref[i + 1].astype(F32).reshape(half, 8, 128)
        a, b = pair_rows(a, b)
        old = jnp.stack([a, b], axis=1).reshape(n, 8, 128)
        mid = (old + mean).reshape(n * 8, 128).astype(BF16)
        normed = layer_norm(mid.astype(F32)).astype(BF16)
        hidden = jnp.maximum(mm(normed, wpu_v[...]), 0.0).astype(BF16)
        new = mid.astype(F32) + mm(hidden, wpd_v[...])
        new = new.reshape(half, 2, 8, 128)
        a, b = pair_rows(new[:, 0], new[:, 1])
        pair_out[i] = a.reshape(cols, 128).astype(BF16)
        pair_out[i + 1] = b.reshape(cols, 128).astype(BF16)

    home.wait()
    drain(msa_out.at[pl.ds(0, (n - 1) * OWNED)], o_recv)
    for c in range(OWNED):
        drain(xcol.at[c, pl.ds(0, (n - 1) * shard_rows)], in_send.at[c])
    drain(ycol.at[:, pl.ds(0, (n - 1) * shard_rows)], o_send)
    drain(rbuf.at[:, pl.ds(0, (4 * lines - 1) * 32)], r_send)
    for r in range(res_n):

        @pl.when(jnp.logical_not(jnp.logical_and(q_row == me, my_res == r)))
        def _(r=r):
            drain(lsend, l_send.at[r])


def per_device(
    homolog_embedding,
    pair_features,
    row_present_mask,
    residue_keep_mask,
    query_weight,
    key_weight,
    content_matrix,
    sigmoid_switch_matrix,
    focus_merge_matrix,
    widening_matrix,
    narrowing_matrix,
    first_factor_matrix,
    second_factor_matrix,
    outer_product_weight,
    outer_product_bias,
    pair_up_weight,
    pair_down_weight,
):
    n = lax.axis_size("seq")
    res_n = lax.axis_size("res")
    shard_rows, cols, width = homolog_embedding.shape
    row_span, _, c_z = pair_features.shape
    rows = shard_rows * n
    assert cols == OWNED * n and n % 4 == 0 and n % res_n == 0
    hidden = widening_matrix.shape[1]
    x = homolog_embedding.transpose(1, 0, 2)
    w1 = jnp.tile(first_factor_matrix, (1, OWNED))
    w2 = second_factor_matrix.T.reshape(COUPLING_DIM // PACK, PACK, 1, width)
    w2 = jnp.broadcast_to(
        w2.transpose(1, 0, 2, 3), (PACK, COUPLING_DIM // PACK, OWNED, width)
    ).reshape(128, width)
    wo = outer_product_weight.reshape(COUPLING_DIM, 4, 2, PACK, c_z)
    wo = wo.transpose(1, 3, 0, 2, 4).reshape(4 * PACK * COUPLING_DIM, 2 * c_z)
    vmem = pl.BlockSpec(memory_space=pltpu.VMEM)
    smem = pl.BlockSpec(memory_space=pltpu.SMEM)
    anyw = pl.BlockSpec(memory_space=pl.ANY)
    dma = pltpu.SemaphoreType.DMA
    lines = n // 4
    msa, pair = pl.pallas_call(
        functools.partial(kernel, n, res_n),
        out_shape=(
            jax.ShapeDtypeStruct((cols, shard_rows, width), BF16),
            jax.ShapeDtypeStruct(pair_features.shape, BF16),
        ),
        in_specs=[vmem, vmem, vmem, smem] + [anyw] * 10 + [vmem] + [anyw] * 2,
        out_specs=(vmem, vmem),
        scratch_shapes=[
            pltpu.VMEM((width, 4 * width), BF16),
            pltpu.VMEM(focus_merge_matrix.shape, BF16),
            pltpu.VMEM(widening_matrix.shape, BF16),
            pltpu.VMEM(narrowing_matrix.shape, BF16),
            pltpu.VMEM(w1.shape, BF16),
            pltpu.VMEM(w2.shape, BF16),
            pltpu.VMEM(wo.shape, BF16),
            pltpu.VMEM(pair_up_weight.shape, BF16),
            pltpu.VMEM(pair_down_weight.shape, BF16),
            pltpu.VMEM((OWNED, rows, width), BF16),
            pltpu.VMEM((OWNED, rows, width), BF16),
            pltpu.VMEM((OWNED, rows, width), BF16),
            pltpu.VMEM((rows, 128), BF16),
            pltpu.VMEM((res_n, rows, 128), BF16),
            pltpu.VMEM((PACK, rows, row_span * 128), BF16),
            pltpu.VMEM((PACK, n * 32, rows), BF16),
            pltpu.VMEM((n, 8, 128), F32),
            dma((12,)),
            dma,
            dma((OWNED,)),
            dma((OWNED,)),
            dma((res_n,)),
            dma((res_n,)),
            dma,
            dma((lines,)),
            dma((lines,)),
            dma((2, lines)),
            dma,
            dma,
        ],
        compiler_params=pltpu.CompilerParams(
            has_side_effects=True, vmem_limit_bytes=60 * 1024 * 1024
        ),
    )(
        x,
        pair_features,
        row_present_mask.reshape(1, rows),
        residue_keep_mask,
        query_weight,
        key_weight,
        content_matrix,
        sigmoid_switch_matrix,
        focus_merge_matrix,
        widening_matrix,
        narrowing_matrix,
        w1,
        w2,
        wo,
        outer_product_bias.reshape(1, c_z),
        pair_up_weight,
        pair_down_weight,
    )
    return (msa.transpose(1, 0, 2), pair)


def solution(mesh):
    placed = (P("seq", "res", None), P("seq", "res", None)) + (P(),) * 15
    return jax.shard_map(
        per_device,
        mesh=mesh,
        in_specs=placed,
        out_specs=(P("seq", "res", None), P("seq", "res", None)),
        check_vma=False,
    )
```

```python
import functools
import math

import jax
import jax.numpy as jnp
from jax import lax
from jax.experimental import pallas as pl
from jax.experimental.pallas import tpu as pltpu
from jax.sharding import PartitionSpec as P

FOCUS_NUMBER = 8
FOCUS_BREADTH = 32
COUPLING_DIM = 32
OWNED = 4
PACK = 4

epsilon = 1e-05
mask_fill = 1000000000.0
F32 = jnp.float32
BF16 = jnp.bfloat16


def layer_norm(values):
    centre = values - jnp.mean(values, axis=-1, keepdims=True)
    spread = jnp.mean(centre * centre, axis=-1, keepdims=True)
    return centre * lax.rsqrt(spread + epsilon)


def mm(a, b):
    return jnp.dot(a, b, preferred_element_type=F32)


def mm_nt(a, b):
    return lax.dot_general(a, b, (((1,), (1,)), ((), ())), preferred_element_type=F32)


def kernel(
    n,
    res_n,
    x_ref,
    pair_ref,
    rowm_ref,
    keep_ref,
    wq,
    wk,
    wv,
    wg,
    wm,
    wu,
    wn,
    w1,
    w2,
    wo,
    bias_ref,
    wpu,
    wpd,
    msa_out,
    pair_out,
    proj_w,
    wm_v,
    wu_v,
    wn_v,
    w1_v,
    w2_v,
    wo_v,
    wpu_v,
    wpd_v,
    xcol,
    ycol,
    n3,
    lsend,
    lbuf,
    lexp,
    rbuf,
    keepj,
    w_sem,
    own_sem,
    in_send,
    in_recv,
    l_send,
    l_recv,
    r_send,
    rz_recv,
    ry_recv,
    rc_recv,
    o_send,
    o_recv,
):
    me = lax.axis_index("seq")
    my_res = lax.axis_index("res")
    cols, shard_rows, width = x_ref.shape
    rows = n * shard_rows
    lines = n // 4
    row_span = pair_ref.shape[0]

    def remote(src, dst, send, recv, where):
        return pltpu.make_async_remote_copy(
            src_ref=src,
            dst_ref=dst,
            send_sem=send,
            recv_sem=recv,
            device_id=where,
            device_id_type=pl.DeviceIdType.MESH,
        )

    def at(s):
        return (s, my_res)

    def drain(ref, sem):
        pltpu.make_async_copy(ref, ref, sem).wait()

    my_rows = pl.ds(pl.multiple_of(me * shard_rows, shard_rows), shard_rows)
    for c in range(OWNED):

        @pl.loop(1, n)
        def _(k, c=c):
            dst = lax.rem(me + k, n)
            remote(
                x_ref.at[dst * OWNED + c],
                xcol.at[c, my_rows],
                in_send.at[c],
                in_recv.at[c],
                at(dst),
            ).start()

    own = pltpu.make_async_copy(
        x_ref.at[pl.ds(me * OWNED, OWNED)], xcol.at[:, my_rows], own_sem
    )
    own.start()
    fetches = [
        (wq, proj_w.at[:, 0:width]),
        (wk, proj_w.at[:, width : 2 * width]),
        (wv, proj_w.at[:, 2 * width : 3 * width]),
        (wg, proj_w.at[:, 3 * width : 4 * width]),
        (wm, wm_v),
        (wu, wu_v),
        (wn, wn_v),
        (w1, w1_v),
        (w2, w2_v),
        (wo, wo_v),
        (wpu, wpu_v),
        (wpd, wpd_v),
    ]
    fetches = [pltpu.make_async_copy(s, d, w_sem.at[i]) for i, (s, d) in enumerate(fetches)]
    for f in fetches:
        f.start()

    sub = lax.broadcasted_iota(jnp.int32, (8, 128), 0)
    for d in range(n):
        flags = [
            keep_ref[my_res * cols + d * OWNED + m].astype(F32) for m in range(OWNED)
        ]
        tile = jnp.full((8, 128), flags[0], F32)
        for m in range(1, OWNED):
            tile = jnp.where(lax.rem(sub, OWNED) == m, flags[m], tile)
        keepj[d] = tile

    row_flags = rowm_ref[...].astype(F32)
    bias = (row_flags - 1.0) * mask_fill
    lane = lax.broadcasted_iota(jnp.int32, (1, width), 1)
    head_masks = [
        (lane // FOCUS_BREADTH == h).astype(F32).astype(BF16) for h in range(FOCUS_NUMBER)
    ]
    scaling = 1.0 / math.sqrt(FOCUS_BREADTH)
    own.wait()
    for f in fetches:
        f.wait()

    def column(c, carry):
        drain(xcol.at[c, pl.ds(0, (n - 1) * shard_rows)], in_recv.at[c])
        inputs = xcol[c].astype(F32)
        normed = layer_norm(inputs).astype(BF16)
        q = (mm(normed, proj_w[:, 0:width]) * scaling).astype(BF16)
        k = mm(normed, proj_w[:, width : 2 * width]).astype(BF16)
        v = mm(normed, proj_w[:, 2 * width : 3 * width]).astype(BF16)
        top = jnp.zeros((rows, width), F32)
        low = jnp.zeros((rows, width), F32)
        for h in range(FOCUS_NUMBER):
            scores = mm_nt(q * head_masks[h], k) + bias
            peak = jnp.max(scores, axis=-1, keepdims=True)
            e = jnp.exp(scores - peak).astype(BF16)
            top = top + mm(e, v * head_masks[h])
            low = low + mm(e, jnp.broadcast_to(head_masks[h], (rows, width)))
        gate = jax.nn.sigmoid(mm(normed, proj_w[:, 3 * width : 4 * width]))
        gated = (gate * (top / low)).astype(BF16)
        after = (inputs + mm(gated, wm_v[...])).astype(BF16)
        normed_two = layer_norm(after.astype(F32)).astype(BF16)
        hidden = jnp.maximum(mm(normed_two, wu_v[...]), 0.0).astype(BF16)
        updated = (after.astype(F32) + mm(hidden, wn_v[...])).astype(BF16)
        ycol[c] = updated
        n3[c] = layer_norm(updated.astype(F32)).astype(BF16)

        @pl.loop(1, n)
        def _(k):
            dst = lax.rem(me + k, n)
            remote(
                ycol.at[c, pl.ds(pl.multiple_of(dst * shard_rows, shard_rows), shard_rows)],
                msa_out.at[me * OWNED + c],
                o_send,
                o_recv,
                at(dst),
            ).start()

        return carry

    lax.fori_loop(0, OWNED, column, 0)

    lanes = lax.broadcasted_iota(jnp.int32, (1, 128), 1)
    tall = lax.broadcasted_iota(jnp.int32, (128, width), 0)
    left = jnp.zeros((rows, 128), F32)
    right = jnp.zeros((128, rows), F32)
    for c in range(OWNED):
        here = (lanes // COUPLING_DIM == c).astype(F32).astype(BF16)
        left = left + mm(n3[c], w1_v[...] * here)
        there = (lax.rem(tall, OWNED) == c).astype(F32).astype(BF16)
        right = right + mm_nt(w2_v[...] * there, n3[c])
    right = (right * row_flags).astype(BF16)
    my_block = pl.ds(pl.multiple_of(me * 32, 32), 32)
    for k in range(PACK):
        rbuf[k, my_block, :] = right[k * 32 : (k + 1) * 32]
    lsend[...] = left.astype(BF16)

    line = me // 4
    spot = lax.rem(me, 4)
    core = lax.rem(me, 2)
    y_pair = line * 4 + lax.rem(spot + 2, 4)
    c_pair = me + 1 - 2 * core

    def pass_on(block, sem, to):
        part = rbuf.at[:, pl.ds(pl.multiple_of(block * 32, 32), 32)]
        remote(part, part, r_send, sem, at(to)).start()

    def got(block, sem):
        drain(rbuf.at[:, pl.ds(pl.multiple_of(block * 32, 32), 32)], sem)

    def line_block(k):
        z = lax.rem(line + lines - k, lines)
        return z, z * 4 + spot, z * 4 + lax.rem(spot + 2, 4)

    for k in range(1, lines):
        pass_on(me, rz_recv.at[line], lax.rem(line + k, lines) * 4 + spot)
    pass_on(me, ry_recv.at[line], y_pair)
    pass_on(me, rc_recv.at[0, line], c_pair)

    q_row = my_res * (n // res_n) + me // res_n
    slot = lax.rem(me, res_n)
    for r in range(res_n):
        local = jnp.logical_and(q_row == me, my_res == r)

        @pl.when(local)
        def _():
            pltpu.make_async_copy(lsend, lbuf.at[slot], l_recv.at[slot]).start()

        @pl.when(jnp.logical_not(local))
        def _(r=r):
            remote(lsend, lbuf.at[slot], l_send.at[r], l_recv.at[slot], (q_row, r)).start()

    for k in range(1, lines):
        z, block, _ = line_block(k)
        got(block, rz_recv.at[z])
        pass_on(block, ry_recv.at[z], y_pair)
        pass_on(block, rc_recv.at[0, z], c_pair)
    for k in range(lines):
        z, _, block = line_block(k)
        got(block, ry_recv.at[z])
        pass_on(block, rc_recv.at[1, z], c_pair)

    home = pltpu.make_async_copy(
        ycol.at[:, my_rows], msa_out.at[pl.ds(me * OWNED, OWNED)], own_sem
    )
    home.start()

    for t in range(res_n):
        drain(lbuf.at[t], l_recv.at[t])
        block = lbuf[t].astype(F32)
        turned = [block] + [pltpu.roll(block, 32 * a, 1) for a in range(1, PACK)]
        for k in range(PACK):
            inside = lanes // COUPLING_DIM == k
            for m in range(OWNED):
                tile = jnp.where(inside, turned[(k - m) % PACK], 0.0).astype(BF16)
                i = t * OWNED + m
                lexp[k, :, i * 128 : (i + 1) * 128] = tile
    for k in range(lines):
        z, block, other = line_block(k)
        got(z * 4 + lax.rem(spot, 4) + 1 - 2 * core, rc_recv.at[0, z])
        got(z * 4 + lax.rem(spot + 2, 4) + 1 - 2 * core, rc_recv.at[1, z])

    live = jnp.sum(row_flags, axis=-1, keepdims=True)
    sub3 = lax.broadcasted_iota(jnp.int32, (1, 8, 128), 1)
    first = sub3 < 4
    flags_j = keepj[...]
    add_bias = bias_ref[...].reshape(1, 1, 128)
    half = n // 2

    def pair_rows(a, b):
        return jnp.where(first, a, pltpu.roll(b, 4, 1)), jnp.where(first, pltpu.roll(a, 4, 1), b)

    for ip in range(row_span // 2):
        outer = jnp.zeros((n * 32, 256), F32)
        for k in range(PACK):
            outer = outer + mm(rbuf[k], lexp[k, :, ip * 256 : (ip + 1) * 256])
        outer = outer.reshape(n, 4, 8, 256)
        sums = []
        for p in range(2):
            total = jnp.zeros((n * 8, 256), F32)
            for g in range(4):
                piece = outer[:, g, :, p * 128 : (p + 1) * 128].reshape(n * 8, 128).astype(BF16)
                total = total + mm(piece, wo_v[g * 128 : (g + 1) * 128, :])
            total = total.reshape(n, 8, 256)
            total = jnp.where(first, total[:, :, :128], total[:, :, 128:])
            sums.append(total + pltpu.roll(total, 4, 1))
        total = jnp.where(first, sums[0], sums[1])
        i = 2 * ip
        keep_a = keep_ref[me * row_span + i].astype(F32)
        keep_b = keep_ref[me * row_span + i + 1].astype(F32)
        flags = jnp.where(first, keep_a, keep_b) * flags_j
        norm = live.reshape(1, 1, 1) * flags
        mean = (total * flags + add_bias) / jnp.maximum(norm, 1.0)
        a = pair_ref[i].astype(F32).reshape(half, 8, 128)
        b = pair_ref[i + 1].astype(F32).reshape(half, 8, 128)
        a, b = pair_rows(a, b)
        old = jnp.stack([a, b], axis=1).reshape(n, 8, 128)
        mid = (old + mean).reshape(n * 8, 128).astype(BF16)
        normed = layer_norm(mid.astype(F32)).astype(BF16)
        hidden = jnp.maximum(mm(normed, wpu_v[...]), 0.0).astype(BF16)
        new = mid.astype(F32) + mm(hidden, wpd_v[...])
        new = new.reshape(half, 2, 8, 128)
        a, b = pair_rows(new[:, 0], new[:, 1])
        pair_out[i] = a.reshape(cols, 128).astype(BF16)
        pair_out[i + 1] = b.reshape(cols, 128).astype(BF16)

    home.wait()
    drain(msa_out.at[pl.ds(0, (n - 1) * OWNED)], o_recv)
    for c in range(OWNED):
        drain(xcol.at[c, pl.ds(0, (n - 1) * shard_rows)], in_send.at[c])
    drain(ycol.at[:, pl.ds(0, (n - 1) * shard_rows)], o_send)
    drain(rbuf.at[:, pl.ds(0, (4 * lines - 1) * 32)], r_send)
    for r in range(res_n):

        @pl.when(jnp.logical_not(jnp.logical_and(q_row == me, my_res == r)))
        def _(r=r):
            drain(lsend, l_send.at[r])


def per_device(
    homolog_embedding,
    pair_features,
    row_present_mask,
    residue_keep_mask,
    query_weight,
    key_weight,
    content_matrix,
    sigmoid_switch_matrix,
    focus_merge_matrix,
    widening_matrix,
    narrowing_matrix,
    first_factor_matrix,
    second_factor_matrix,
    outer_product_weight,
    outer_product_bias,
    pair_up_weight,
    pair_down_weight,
):
    n = lax.axis_size("seq")
    res_n = lax.axis_size("res")
    shard_rows, cols, width = homolog_embedding.shape
    row_span, _, c_z = pair_features.shape
    rows = shard_rows * n
    assert cols == OWNED * n and n % 4 == 0 and n % res_n == 0
    hidden = widening_matrix.shape[1]
    x = homolog_embedding.transpose(1, 0, 2)
    w1 = jnp.tile(first_factor_matrix, (1, OWNED))
    w2 = second_factor_matrix.T.reshape(COUPLING_DIM // PACK, PACK, 1, width)
    w2 = jnp.broadcast_to(
        w2.transpose(1, 0, 2, 3), (PACK, COUPLING_DIM // PACK, OWNED, width)
    ).reshape(128, width)
    wo = outer_product_weight.reshape(COUPLING_DIM, 4, 2, PACK, c_z)
    wo = wo.transpose(1, 3, 0, 2, 4).reshape(4 * PACK * COUPLING_DIM, 2 * c_z)
    vmem = pl.BlockSpec(memory_space=pltpu.VMEM)
    smem = pl.BlockSpec(memory_space=pltpu.SMEM)
    anyw = pl.BlockSpec(memory_space=pl.ANY)
    dma = pltpu.SemaphoreType.DMA
    lines = n // 4
    msa, pair = pl.pallas_call(
        functools.partial(kernel, n, res_n),
        out_shape=(
            jax.ShapeDtypeStruct((cols, shard_rows, width), BF16),
            jax.ShapeDtypeStruct(pair_features.shape, BF16),
        ),
        in_specs=[vmem, vmem, vmem, smem] + [anyw] * 10 + [vmem] + [anyw] * 2,
        out_specs=(vmem, vmem),
        scratch_shapes=[
            pltpu.VMEM((width, 4 * width), BF16),
            pltpu.VMEM(focus_merge_matrix.shape, BF16),
            pltpu.VMEM(widening_matrix.shape, BF16),
            pltpu.VMEM(narrowing_matrix.shape, BF16),
            pltpu.VMEM(w1.shape, BF16),
            pltpu.VMEM(w2.shape, BF16),
            pltpu.VMEM(wo.shape, BF16),
            pltpu.VMEM(pair_up_weight.shape, BF16),
            pltpu.VMEM(pair_down_weight.shape, BF16),
            pltpu.VMEM((OWNED, rows, width), BF16),
            pltpu.VMEM((OWNED, rows, width), BF16),
            pltpu.VMEM((OWNED, rows, width), BF16),
            pltpu.VMEM((rows, 128), BF16),
            pltpu.VMEM((res_n, rows, 128), BF16),
            pltpu.VMEM((PACK, rows, row_span * 128), BF16),
            pltpu.VMEM((PACK, n * 32, rows), BF16),
            pltpu.VMEM((n, 8, 128), F32),
            dma((12,)),
            dma,
            dma((OWNED,)),
            dma((OWNED,)),
            dma((res_n,)),
            dma((res_n,)),
            dma,
            dma((lines,)),
            dma((lines,)),
            dma((2, lines)),
            dma,
            dma,
        ],
        compiler_params=pltpu.CompilerParams(
            has_side_effects=True, vmem_limit_bytes=60 * 1024 * 1024
        ),
    )(
        x,
        pair_features,
        row_present_mask.reshape(1, rows),
        residue_keep_mask,
        query_weight,
        key_weight,
        content_matrix,
        sigmoid_switch_matrix,
        focus_merge_matrix,
        widening_matrix,
        narrowing_matrix,
        w1,
        w2,
        wo,
        outer_product_bias.reshape(1, c_z),
        pair_up_weight,
        pair_down_weight,
    )
    return (msa.transpose(1, 0, 2), pair)


def solution(mesh):
    placed = (P("seq", "res", None), P("seq", "res", None)) + (P(),) * 15
    return jax.shard_map(
        per_device,
        mesh=mesh,
        in_specs=placed,
        out_specs=(P("seq", "res", None), P("seq", "res", None)),
        check_vma=False,
    )
```
